32 devices in a mesh: freq: 16 (over z, y, x), depth: 2 (over core).
Axes of the slice: x: 2, y: 2, z: 4, core: 2. Of those that a mesh axis runs over, the one named last changes fastest.
Arguments:
- pressure_field: bfloat16 [8192, 4096], P('depth', 'freq'), may hold values from -6 to 6
- block_main: bfloat16 [8192, 3, 2, 128], P('depth'), may hold values from -0.15625 to 0.15625
- block_coupled: bfloat16 [8192, 3, 2, 128], P('depth'), may hold values from -0.15625 to 0.15625
- coupling: float32 [4096], P('freq'), may hold values from -3 to 3
- frequencies: float32 [2048], replicated, may hold values from 1 to 1024
- receivers: int32 [512], replicated, may hold values from 0 to 8191
- floors: int32 [4], replicated, may hold values from 2048 to 8191
Outputs:
- series: float32 [512, 2048], P('depth', 'freq')
The draws below stay inside these ranges and needn't reach their ends.
Inputs may be any that keep to these rules, and one draw needn't show every extreme that they name: `receivers`: any depth cells, repeats possible.
All inputs are finite; a program needn't handle non-finite values.
Results may differ from the reference program's by a relative error of at most 0.0061.
Values may be sent and summed in bfloat16 or wider, within the bound.
A program may use at most 256 MiB of HBM per device.

```python
import math
import jax
import jax.numpy as jnp
from jax import lax

NZ = 8192
BS = 128
NT = 2048
R = 512
STEPS = 4
F_DEV = 128
F = 2048
N_FREQ = 16


def touch_ends(array, key, smallest, largest):
    index_at = [jax.random.randint(jax.random.fold_in(key, axis), (), 0, length) for axis, length in enumerate(array.shape)]
    main_axis = array.shape.index(max(array.shape))
    next_to = index_at[:main_axis] + [(index_at[main_axis] + 1) % array.shape[main_axis]] + index_at[main_axis + 1:]
    return array.at[tuple(index_at)].set(smallest).at[tuple(next_to)].set(largest)


def levels(own_key, shape, cuts, least, top_value):
    level = 1.0
    for position, blocks in cuts:
        draws = jax.random.uniform(jax.random.fold_in(jax.random.fold_in(own_key, 6), position), (blocks,), jnp.float32, least / len(cuts), top_value / len(cuts))
        level = level * jnp.repeat(jnp.exp(draws), shape[position] // blocks).reshape((-1,) + (1,) * (len(shape) - 1 - position))
    return level


def gaussian(stream_key, dims, scale, reach, split=(), held_as=jnp.bfloat16):
    entries = scale * jax.random.normal(stream_key, dims, jnp.float32)
    if split:
        entries = entries * levels(stream_key, dims, split, -0.22, 0.18)
    return jnp.clip(entries, -reach, reach).astype(held_as)


def setup_inputs(seed: int = 0) -> dict:
    streams_of = jax.random.split(jax.random.key(seed), 8)
    return {
        "pressure_field": gaussian(streams_of[0], (NZ, 2 * F), 1.0, 6.0, ((0, 2), (1, 16))),
        "block_main": gaussian(streams_of[1], (NZ, 3, 2, BS), (12 * BS) ** -0.5, 0.15625, ((0, 2),)),
        "block_coupled": gaussian(streams_of[2], (NZ, 3, 2, BS), (12 * BS) ** -0.5, 0.15625, ((0, 2),)),
        "coupling": gaussian(streams_of[3], (2 * F,), 0.5, 3.0, ((0, 16),), jnp.float32),
        "frequencies": jnp.clip(jax.random.uniform(streams_of[4], (F,), jnp.float32, 1.0, 1024.0), 1.0, 1024.0),
        "receivers": touch_ends(jax.random.randint(streams_of[5], (R,), 0, NZ), jax.random.fold_in(streams_of[5], 1), 0, NZ - 1).astype(jnp.int32),
        "floors": touch_ends(jax.random.randint(streams_of[6], (STEPS,), NZ // 4, NZ), jax.random.fold_in(streams_of[6], 1), NZ // 4, NZ - 1).astype(jnp.int32),
    }


def apply_blocks(blocks, padded):
    block_count = blocks.shape[0]
    width = padded.shape[1]
    stacked = padded.reshape(block_count + 2, BS, width)
    neighbours = jnp.stack([stacked[:-2], stacked[1:-1], stacked[2:]], axis=1)
    product = jnp.einsum('bikrj,bkjc->rbic', blocks, neighbours, precision=lax.Precision.HIGHEST)
    real_part = product[0].reshape(block_count * BS, width)
    imag_part = product[1].reshape(block_count * BS, width // 2, 2)
    rotated = jnp.stack([-imag_part[..., 1], imag_part[..., 0]], axis=-1).reshape(block_count * BS, width)
    return real_part + rotated

def couple_terms(values, weights):
    height = values.shape[0]
    paired = values.reshape(height, -1, 2)
    wpair = weights.reshape(-1, 2)
    real_part = wpair[:, 0] * paired[..., 0] - wpair[:, 1] * paired[..., 1]
    imag_part = wpair[:, 0] * paired[..., 1] + wpair[:, 1] * paired[..., 0]
    return jnp.stack([real_part, imag_part], axis=-1).reshape(height, -1)

def make_basis(freq_values, sample_times):
    phase = jnp.mod(freq_values[:, None] * sample_times[None, :], jnp.float32(NT)) / jnp.float32(NT)
    angle = 2.0 * math.pi * phase
    stacked = jnp.stack([jnp.cos(angle), -jnp.sin(angle)], axis=1)
    return stacked.reshape(2 * freq_values.shape[0], sample_times.shape[0]).astype(jnp.bfloat16)

def reference(pressure_field, block_main, block_coupled, coupling, frequencies, receivers, floors):
    block_count = NZ // BS
    main_blocks = block_main.astype(jnp.float32).reshape(block_count, BS, 3, 2, BS)
    side_blocks = block_coupled.astype(jnp.float32).reshape(block_count, BS, 3, 2, BS)
    grouped = pressure_field.reshape(NZ, N_FREQ, 2 * F_DEV).transpose(1, 0, 2)
    pairs = coupling.reshape(N_FREQ, 2 * F_DEV)
    freq_groups = frequencies.reshape(N_FREQ, F_DEV)
    depth_index = jnp.arange(NZ, dtype=jnp.int32)
    sample_times = jnp.arange(NT, dtype=jnp.float32)

    def one_group(running, group_items):
        columns, weights, freq_values = group_items
        for step in range(STEPS):
            padded = jnp.pad(columns.astype(jnp.float32), ((BS, BS), (0, 0)))
            combined = apply_blocks(main_blocks, padded) + couple_terms(apply_blocks(side_blocks, padded), weights)
            damping = jnp.where(depth_index >= floors[step], 0.5, 1.0).astype(jnp.float32)
            columns = (damping[:, None] * combined).astype(jnp.bfloat16)
        picked = jnp.take(columns, receivers, axis=0)
        basis_table = make_basis(freq_values, sample_times)
        return (running + jnp.dot(picked, basis_table, preferred_element_type=jnp.float32), None)
    running, _ = lax.scan(one_group, jnp.zeros((R, NT), jnp.float32), (grouped, pairs, freq_groups))
    return running * (1.0 / math.sqrt(F))
```

```python
import functools
import math

import jax
import jax.numpy as jnp
from jax import lax
from jax.experimental import pallas as pl
from jax.experimental.pallas import tpu as pltpu
from jax.sharding import PartitionSpec as P

NT = 2048
STEPS = 4

COS_TERMS = (1.0, -19.739208221435547, 64.93939208984375, -85.45665740966797,
             60.242130279541016, -26.4046688079834, 7.800131320953369, -1.453112244606018)
SIN_TERMS = (6.2831854820251465, -41.34170150756836, 81.6052474975586, -76.70580291748047,
             42.05775451660156, -15.086565017700195, 3.7813189029693604, -0.6207787394523621)

MESH = pl.DeviceIdType.MESH
F32 = jnp.float32
BF16 = jnp.bfloat16
KC = 6
GROUP = 4


def poly(terms, z):
    total = jnp.full_like(z, terms[-1])
    for term in terms[-2::-1]:
        total = total * z + F32(term)
    return total


def kernel(depth_n, freq_n, near, factor, chunks,
           field, main_hbm, side_hbm, coupling, freqs, receivers, floors, out,
           fbuf, raw_main, raw_side, spread, ops, w_even, w_odd, final, halo, rows_f32, pick_out, pick_in,
           gathered, basis, kept, part_out, part_in,
           field_sem, load_sem, halo_send, halo_recv, pick_send, pick_recv, ag_send, ag_recv, rs_send, rs_recv):
    rows, width = fbuf.shape
    half = width // 2
    nb, _, bw, bs = ops.shape
    groups = nb // GROUP
    far = freq_n // near
    here, times = out.shape
    wide = NT // near
    me_d = lax.axis_index("depth")
    me_f = lax.axis_index("freq")
    me_near = lax.rem(me_f, near)
    me_far = me_f // near
    first_row = me_d * rows
    has_above = me_d > 0
    has_below = me_d < depth_n - 1
    w_bufs = (w_even, w_odd)

    field_copy = pltpu.make_async_copy(field, fbuf, field_sem)
    field_copy.start()
    span = GROUP * bs * KC

    def load_copy(which, grp):
        src, dst = ((main_hbm, raw_main), (side_hbm, raw_side))[which]
        at = pl.ds(grp * span, span)
        return pltpu.make_async_copy(src.at[at], dst.at[at], load_sem.at[which, grp])

    for grp in range(groups):
        for which in range(2):
            load_copy(which, grp).start()

    near_peers = []
    for off in range(1, near):
        peer = me_f
        for bit in range(near.bit_length() - 1):
            if off >> bit & 1:
                mine = lax.rem(me_f // (1 << bit), 2)
                peer = peer + (1 - 2 * mine) * (1 << bit)
        near_peers.append(peer)
    far_peers = [lax.rem(me_far + off, far) * near + me_near for off in range(1, far)]
    barrier = pltpu.get_barrier_semaphore()
    for off in range(1, depth_n):
        pl.semaphore_signal(barrier, inc=1, device_id={"depth": lax.rem(me_d + off, depth_n)},
                            device_id_type=MESH)
    for peer in near_peers + far_peers:
        pl.semaphore_signal(barrier, inc=1, device_id={"freq": peer}, device_id_type=MESH)

    lane = lax.broadcasted_iota(jnp.int32, (half, wide), 1)
    owner = lax.rem(lane // times + me_far, far)
    sample = ((owner * near + me_near) * times + lax.rem(lane, times)).astype(F32)
    for slot, peer in enumerate([me_f] + near_peers):
        row = freqs[pl.ds(peer, 1), :]
        column = jnp.broadcast_to(row, (half, half)).T
        for start in range(0, wide, half):
            n = sample[:, start:start + half]
            y = (column[:, :n.shape[1]] * n) * F32(1.0 / NT)
            p = y - jnp.floor(y)
            r = jnp.where(p > 0.5, p - 1.0, p)
            z = r * r
            basis[slot, :half, start:start + half] = poly(COS_TERMS, z).astype(BF16)
            basis[slot, half:, start:start + half] = (-(r * poly(SIN_TERMS, z))).astype(BF16)

    from_col = lax.broadcasted_iota(jnp.int32, (width, width), 0)
    to_col = lax.broadcasted_iota(jnp.int32, (width, width), 1)
    wanted = jnp.where(to_col < half, 2 * to_col, 2 * (to_col - half) + 1)
    order = jnp.where(from_col == wanted, 1.0, 0.0).astype(BF16)

    pairs = jnp.broadcast_to(jnp.concatenate([coupling[0:1, :], coupling[1:2, :]], axis=1), (16, width))
    weights = jnp.zeros((16, width), F32)
    rest = pairs
    for _ in range(3):
        piece = rest.astype(BF16)
        weights = weights + jnp.dot(piece, order, preferred_element_type=F32)
        rest = rest - piece.astype(F32)
    wr = weights[0:1, :half]
    wi = weights[0:1, half:]

    def put_w(dst, b, re, im):
        at = pl.ds(b * bs, bs)
        dst[0, at, :] = re
        dst[1, at, :] = im
        dst[2, at, :] = -im

    field_copy.wait()

    def enter(b):
        at = pl.ds(b * bs, bs)
        got = jnp.dot(fbuf[at, :], order, preferred_element_type=F32).astype(BF16)
        put_w(w_even, b, got[:, :half], got[:, half:])

    for b in [0, nb - 1] + list(range(1, nb - 1)):
        enter(b)

    blank = jnp.zeros(halo.shape[2:], BF16)

    @pl.when(jnp.logical_not(has_above))
    def _():
        for step in range(STEPS):
            halo[step, 0] = blank

    @pl.when(jnp.logical_not(has_below))
    def _():
        for step in range(STEPS):
            halo[step, 1] = blank

    final[:, rows:, :] = jnp.zeros((2, final.shape[1] - rows, half), F32)

    pl.semaphore_wait(barrier, depth_n - 1 + len(near_peers) + len(far_peers))

    def halo_copy(step, side):
        edge = 0 if side == 1 else nb - 1
        to = lax.rem(me_d + (depth_n - 1 if side == 1 else 1), depth_n)
        return pltpu.make_async_remote_copy(
            src_ref=w_bufs[step % 2].at[:, pl.ds(edge * bs, bs)],
            dst_ref=halo.at[step, side],
            send_sem=halo_send.at[step, side],
            recv_sem=halo_recv.at[step, side],
            device_id={"depth": to},
            device_id_type=MESH,
        )

    def halo_start(step):
        if depth_n == 1:
            return

        @pl.when(has_above)
        def _():
            halo_copy(step, 1).start()

        @pl.when(has_below)
        def _():
            halo_copy(step, 0).start()

    def halo_finish(step):
        if depth_n == 1:
            return

        @pl.when(has_above)
        def _():
            halo_copy(step, 1).wait_send()
            halo_copy(step, 0).wait_recv()

        @pl.when(has_below)
        def _():
            halo_copy(step, 0).wait_send()
            halo_copy(step, 1).wait_recv()

    halo_start(0)

    row_iota = lax.broadcasted_iota(jnp.int32, (bs, half), 0)

    def multiply(step, b):
        src = w_bufs[step % 2]
        pieces = []
        for k in range(3):
            at = b + k - 1
            if at < 0:
                re, im, neg = (halo[step, 0, c] for c in range(3))
            elif at >= nb:
                re, im, neg = (halo[step, 1, c] for c in range(3))
            else:
                re, im, neg = (src[c, pl.ds(at * bs, bs), :] for c in range(3))
            pieces.append(jnp.concatenate([re, im], axis=1))
            pieces.append(jnp.concatenate([neg, re], axis=1))
        rhs = jnp.concatenate(pieces, axis=0)
        lhs = jnp.concatenate([ops[b, piece] for piece in range(KC)], axis=1)
        acc = jnp.dot(lhs, rhs, preferred_element_type=F32)
        m, c = acc[:bs], acc[bs:]
        re = m[:, :half] + wr * c[:, :half] - wi * c[:, half:]
        im = m[:, half:] + wr * c[:, half:] + wi * c[:, :half]
        damp = jnp.where(row_iota + (first_row + b * bs) >= floors[step], F32(0.5), F32(1.0))
        re = damp * re
        im = damp * im
        if step == STEPS - 1:
            at = pl.ds(b * bs, bs)
            final[0, at, :] = re
            final[1, at, :] = im
        else:
            put_w(w_bufs[1 - step % 2], b, re.astype(BF16), im.astype(BF16))

    def prepare(b):
        at = pl.ds(b * KC * bs, KC * bs)
        for which, src in enumerate((raw_main, raw_side)):
            slot = (b % 2) * 2 + which
            spread[slot] = src[at, :].astype(F32)
            for piece in range(KC):
                ops[b, piece, which * bs:(which + 1) * bs, :] = spread[
                    slot, pl.ds(piece, bs, stride=KC), :].astype(BF16)

    for grp in range(groups):
        for which in range(2):
            load_copy(which, grp).wait()
        for i in range(GROUP):
            b = grp * GROUP + i
            prepare(b)
            before = b - GROUP
            if before > 0:
                multiply(0, before)
    halo_finish(0)
    multiply(0, 0)
    multiply(0, nb - 1)
    for b in range(nb - GROUP, nb - 1):
        multiply(0, b)
    halo_start(1)
    for step in range(1, STEPS):
        middle = nb // 2
        for b in range(1, middle):
            multiply(step, b)
        halo_finish(step)
        multiply(step, 0)
        multiply(step, nb - 1)
        for b in range(middle, nb - 1):
            multiply(step, b)
        if step + 1 < STEPS:
            halo_start(step + 1)

    def pick(owner):
        def one(j, carry):
            spot = receivers[owner * here + j] - first_row
            spot = jnp.where(jnp.logical_and(spot >= 0, spot < rows), spot, rows)
            for c in range(2):
                rows_f32[c, pl.ds(j, 1), :] = final[c, pl.ds(spot, 1), :]
            return carry
        lax.fori_loop(0, here, one, 0, unroll=16)

    def pick_copy(off):
        return pltpu.make_async_remote_copy(
            src_ref=pick_out.at[off - 1],
            dst_ref=pick_in.at[off - 1],
            send_sem=pick_send.at[off - 1],
            recv_sem=pick_recv.at[off - 1],
            device_id={"depth": lax.rem(me_d + off, depth_n)},
            device_id_type=MESH,
        )

    for off in range(1, depth_n):
        pick(lax.rem(me_d + off, depth_n))
        pick_out[off - 1] = rows_f32[...].astype(BF16)
        pick_copy(off).start()
    pick(me_d)
    for off in range(1, depth_n):
        pick_copy(off).wait()

    def ag_copy(off, chunk):
        start, count = chunks[chunk]
        at = pl.ds(start, count)
        return pltpu.make_async_remote_copy(
            src_ref=gathered.at[0, :, at],
            dst_ref=gathered.at[off, :, at],
            send_sem=ag_send.at[off - 1, chunk],
            recv_sem=ag_recv.at[off - 1, chunk],
            device_id={"freq": near_peers[off - 1]},
            device_id_type=MESH,
        )

    for chunk, (start, count) in enumerate(chunks):
        at = slice(start, start + count)
        mine = rows_f32[:, at, :]
        for off in range(1, depth_n):
            mine = mine + pick_in[off - 1, :, at, :].astype(F32)
        gathered[0, :, at, :] = mine.astype(BF16)
        for off in range(1, near):
            ag_copy(off, chunk).start()

    def rs_copy(off, chunk):
        start, count = chunks[chunk]
        at = pl.ds(start, count)
        return pltpu.make_async_remote_copy(
            src_ref=part_out.at[off - 1, at],
            dst_ref=part_in.at[off - 1, at],
            send_sem=rs_send.at[off - 1, chunk],
            recv_sem=rs_recv.at[off - 1, chunk],
            device_id={"freq": far_peers[off - 1]},
            device_id_type=MESH,
        )

    for chunk, (start, count) in enumerate(chunks):
        at = slice(start, start + count)
        for off in range(1, near):
            ag_copy(off, chunk).wait_recv()
        lhs = jnp.concatenate([gathered[slot, c, at, :] for slot in range(near) for c in range(2)], axis=1)
        rhs = jnp.concatenate([basis[slot] for slot in range(near)], axis=0)
        total = jnp.dot(lhs, rhs, preferred_element_type=F32)
        for off in range(1, far):
            part_out[off - 1, at, :] = total[:, off * times:(off + 1) * times].astype(BF16)
            rs_copy(off, chunk).start()
        kept[at, :] = total[:, :times]
    for chunk, (start, count) in enumerate(chunks):
        at = slice(start, start + count)
        total = kept[at, :]
        for off in range(1, far):
            rs_copy(off, chunk).wait_recv()
            total = total + part_in[off - 1, at, :].astype(F32)
        out[at, :] = total * factor
    for chunk in range(len(chunks)):
        for off in range(1, near):
            ag_copy(off, chunk).wait_send()
        for off in range(1, far):
            rs_copy(off, chunk).wait_send()


def local(depth_n, freq_n, pressure_field, block_main, block_coupled, coupling, frequencies,
          receivers, floors):
    rows, width = pressure_field.shape
    bs = block_main.shape[3]
    half = width // 2
    nb = rows // bs
    near = min(4, freq_n)
    far = freq_n // near
    here = receivers.shape[0] // depth_n
    times = NT // freq_n
    factor = 1.0 / math.sqrt(frequencies.shape[0])
    count = max(here // 4, 16)
    chunks = [(start, count) for start in range(0, here, count)]
    vmem = pl.BlockSpec(memory_space=pltpu.VMEM)
    hbm = pl.BlockSpec(memory_space=pl.ANY)
    smem = pl.BlockSpec(memory_space=pltpu.SMEM)
    away = max(depth_n - 1, 1)
    near_slots, far_slots = max(near - 1, 1), max(far - 1, 1)
    dma = pltpu.SemaphoreType.DMA
    return pl.pallas_call(
        functools.partial(kernel, depth_n, freq_n, near, factor, chunks),
        out_shape=jax.ShapeDtypeStruct((here, times), F32),
        in_specs=[hbm, hbm, hbm, vmem, vmem, smem, smem],
        out_specs=vmem,
        scratch_shapes=[
            pltpu.VMEM((rows, width), BF16),
            pltpu.VMEM((rows * KC, bs), BF16),
            pltpu.VMEM((rows * KC, bs), BF16),
            pltpu.VMEM((4, KC * bs, bs), F32),
            pltpu.VMEM((nb, KC, 2 * bs, bs), BF16),
            pltpu.VMEM((3, rows, half), BF16),
            pltpu.VMEM((3, rows, half), BF16),
            pltpu.VMEM((2, rows + 8, half), F32),
            pltpu.VMEM((STEPS, 2, 3, bs, half), BF16),
            pltpu.VMEM((2, here, half), F32),
            pltpu.VMEM((away, 2, here, half), BF16),
            pltpu.VMEM((away, 2, here, half), BF16),
            pltpu.VMEM((near, 2, here, half), BF16),
            pltpu.VMEM((near, width, NT // near), BF16),
            pltpu.VMEM((here, times), F32),
            pltpu.VMEM((far_slots, here, times), BF16),
            pltpu.VMEM((far_slots, here, times), BF16),
            dma(()),
            dma((2, nb // GROUP)),
            dma((STEPS, 2)),
            dma((STEPS, 2)),
            dma((away,)),
            dma((away,)),
            dma((near_slots, len(chunks))),
            dma((near_slots, len(chunks))),
            dma((far_slots, len(chunks))),
            dma((far_slots, len(chunks))),
        ],
        compiler_params=pltpu.CompilerParams(
            collective_id=0, has_side_effects=True, vmem_limit_bytes=64 * 1024 * 1024 - 128 * 1024
        ),
    )(
        pressure_field,
        block_main.reshape(rows * KC, bs),
        block_coupled.reshape(rows * KC, bs),
        coupling.reshape(2, half),
        frequencies.reshape(freq_n, half),
        receivers,
        floors,
    )


def solution(mesh):
    in_specs = (
        P("depth", "freq"),
        P("depth", None, None, None),
        P("depth", None, None, None),
        P("freq"),
        P(),
        P(),
        P(),
    )
    body = functools.partial(local, mesh.shape["depth"], mesh.shape["freq"])
    return jax.shard_map(body, mesh=mesh, in_specs=in_specs, out_specs=P("depth", "freq"),
                         check_vma=False)
```

```python
import functools
import math

import jax
import jax.numpy as jnp
from jax import lax
from jax.experimental import pallas as pl
from jax.experimental.pallas import tpu as pltpu
from jax.sharding import PartitionSpec as P

NT = 2048
STEPS = 4

COS_TERMS = (1.0, -19.739208221435547, 64.93939208984375, -85.45665740966797,
             60.242130279541016, -26.4046688079834, 7.800131320953369, -1.453112244606018)
SIN_TERMS = (6.2831854820251465, -41.34170150756836, 81.6052474975586, -76.70580291748047,
             42.05775451660156, -15.086565017700195, 3.7813189029693604, -0.6207787394523621)

MESH = pl.DeviceIdType.MESH
F32 = jnp.float32
BF16 = jnp.bfloat16
KC = 6
VMEM_LIMIT = 46 * 1024 * 1024
GROUPS = (4, 4, 4, 4, 4, 4, 4, 4)
MEET = 4
AHEAD = 5
FIELD_PARTS = 4


def poly(terms, z):
    total = jnp.full_like(z, terms[-1])
    for term in terms[-2::-1]:
        total = total * z + F32(term)
    return total


def group_cuts(nb):
    cuts = [0]
    while cuts[-1] < nb:
        cuts.append(min(nb, cuts[-1] + GROUPS[min(len(cuts) - 1, len(GROUPS) - 1)]))
    return cuts


def kernel(depth_n, freq_n, near, factor, chunks,
           field, main_hbm, side_hbm, coupling, freqs, receivers, floors, out,
           fbuf, raw_main, raw_side, ops, w_even, w_odd, final, halo, rows_f32, pick_out, pick_in,
           gathered, basis, kept, part_out, part_in,
           field_sem, load_sem, halo_send, halo_recv, pick_send, pick_recv, ag_send, ag_recv, rs_send, rs_recv):
    rows, width = fbuf.shape
    half = width // 2
    nb, _, bw, bs = ops.shape
    cuts = group_cuts(nb)
    far = freq_n // near
    here, times = out.shape
    wide = NT // near
    me_d = lax.axis_index("depth")
    me_f = lax.axis_index("freq")
    me_near = lax.rem(me_f, near)
    me_far = me_f // near
    first_row = me_d * rows
    has_above = me_d > 0
    has_below = me_d < depth_n - 1
    w_bufs = (w_even, w_odd)

    def field_copy(part):
        at = pl.ds(part * (rows // FIELD_PARTS), rows // FIELD_PARTS)
        return pltpu.make_async_copy(field.at[at], fbuf.at[at], field_sem.at[part])

    for part in range(FIELD_PARTS):
        field_copy(part).start()

    def load_start(grp):
        if grp < len(cuts) - 1:
            for which in range(2):
                load_copy(which, grp).start()

    def load_copy(which, grp):
        src, dst = ((main_hbm, raw_main), (side_hbm, raw_side))[which]
        at = pl.ds(cuts[grp] * bs * KC, (cuts[grp + 1] - cuts[grp]) * bs * KC)
        return pltpu.make_async_copy(src.at[at], dst.at[at], load_sem.at[which, grp])

    load_start(0)

    near_peers = []
    for off in range(1, near):
        peer = me_f
        for bit in range(near.bit_length() - 1):
            if off >> bit & 1:
                mine = lax.rem(me_f // (1 << bit), 2)
                peer = peer + (1 - 2 * mine) * (1 << bit)
        near_peers.append(peer)
    far_peers = [lax.rem(me_far + off, far) * near + me_near for off in range(1, far)]
    barrier = pltpu.get_barrier_semaphore()
    for off in range(1, depth_n):
        pl.semaphore_signal(barrier, inc=1, device_id={"depth": lax.rem(me_d + off, depth_n)},
                            device_id_type=MESH)
    for peer in near_peers + far_peers:
        pl.semaphore_signal(barrier, inc=1, device_id={"freq": peer}, device_id_type=MESH)

    lane = lax.broadcasted_iota(jnp.int32, (half, wide), 1)
    owner = lax.rem(lane // times + me_far, far)
    sample = ((owner * near + me_near) * times + lax.rem(lane, times)).astype(F32)
    for slot, peer in enumerate([me_f] + near_peers):
        row = freqs[pl.ds(peer, 1), :]
        column = jnp.broadcast_to(row, (half, half)).T
        for start in range(0, wide, half):
            n = sample[:, start:start + half]
            y = (column[:, :n.shape[1]] * n) * F32(1.0 / NT)
            p = y - jnp.floor(y)
            r = jnp.where(p > 0.5, p - 1.0, p)
            z = r * r
            basis[slot, :half, start:start + half] = poly(COS_TERMS, z).astype(BF16)
            basis[slot, half:, start:start + half] = (-(r * poly(SIN_TERMS, z))).astype(BF16)

    for grp in range(1, AHEAD):
        load_start(grp)

    from_col = lax.broadcasted_iota(jnp.int32, (width, width), 0)
    to_col = lax.broadcasted_iota(jnp.int32, (width, width), 1)
    wanted = jnp.where(to_col < half, 2 * to_col, 2 * (to_col - half) + 1)
    order = jnp.where(from_col == wanted, 1.0, 0.0).astype(BF16)

    pairs = jnp.broadcast_to(jnp.concatenate([coupling[0:1, :], coupling[1:2, :]], axis=1), (16, width))
    weights = jnp.zeros((16, width), F32)
    rest = pairs
    for _ in range(3):
        piece = rest.astype(BF16)
        weights = weights + jnp.dot(piece, order, preferred_element_type=F32)
        rest = rest - piece.astype(F32)
    wr = weights[0:1, :half]
    wi = weights[0:1, half:]

    def put_w(dst, b, re, im):
        at = pl.ds(b * bs, bs)
        dst[0, at, :] = re
        dst[1, at, :] = im
        dst[2, at, :] = -im

    for part in range(FIELD_PARTS):
        field_copy(part).wait()

    def enter(b):
        at = pl.ds(b * bs, bs)
        got = jnp.dot(fbuf[at, :], order, preferred_element_type=F32).astype(BF16)
        put_w(w_even, b, got[:, :half], got[:, half:])

    for b in [0, nb - 1] + list(range(1, nb - 1)):
        enter(b)

    blank = jnp.zeros(halo.shape[2:], BF16)

    @pl.when(jnp.logical_not(has_above))
    def _():
        for step in range(STEPS):
            halo[step, 0] = blank

    @pl.when(jnp.logical_not(has_below))
    def _():
        for step in range(STEPS):
            halo[step, 1] = blank

    final[:, rows:, :] = jnp.zeros((2, final.shape[1] - rows, half), F32)

    def halo_copy(step, side):
        edge = 0 if side == 1 else nb - 1
        to = lax.rem(me_d + (depth_n - 1 if side == 1 else 1), depth_n)
        return pltpu.make_async_remote_copy(
            src_ref=w_bufs[step % 2].at[:, pl.ds(edge * bs, bs)],
            dst_ref=halo.at[step, side],
            send_sem=halo_send.at[step, side],
            recv_sem=halo_recv.at[step, side],
            device_id={"depth": to},
            device_id_type=MESH,
        )

    def halo_start(step):
        if depth_n == 1:
            return

        @pl.when(has_above)
        def _():
            halo_copy(step, 1).start()

        @pl.when(has_below)
        def _():
            halo_copy(step, 0).start()

    def halo_finish(step):
        if depth_n == 1:
            return

        @pl.when(has_above)
        def _():
            halo_copy(step, 1).wait_send()
            halo_copy(step, 0).wait_recv()

        @pl.when(has_below)
        def _():
            halo_copy(step, 0).wait_send()
            halo_copy(step, 1).wait_recv()

    row_iota = lax.broadcasted_iota(jnp.int32, (bs, half), 0)

    def multiply(step, b):
        src = w_bufs[step % 2]
        pieces = []
        for k in range(3):
            at = b + k - 1
            if at < 0:
                re, im, neg = (halo[step, 0, c] for c in range(3))
            elif at >= nb:
                re, im, neg = (halo[step, 1, c] for c in range(3))
            else:
                re, im, neg = (src[c, pl.ds(at * bs, bs), :] for c in range(3))
            pieces.append(jnp.concatenate([re, im], axis=1))
            pieces.append(jnp.concatenate([neg, re], axis=1))
        rhs = jnp.concatenate(pieces, axis=0)
        if step == 0:
            lhs = jnp.concatenate([
                jnp.concatenate([raw[pl.ds(b * KC * bs + piece, bs, stride=KC), :] for piece in range(KC)], axis=1)
                for raw in (raw_main, raw_side)
            ], axis=0)
            for piece in range(KC):
                ops[b, piece] = lhs[:, piece * bs:(piece + 1) * bs]
        else:
            lhs = jnp.concatenate([ops[b, piece] for piece in range(KC)], axis=1)
        acc = jnp.dot(lhs, rhs, preferred_element_type=F32)
        m, c = acc[:bs], acc[bs:]
        re = m[:, :half] + wr * c[:, :half] - wi * c[:, half:]
        im = m[:, half:] + wr * c[:, half:] + wi * c[:, :half]
        damp = jnp.where(row_iota + (first_row + b * bs) >= floors[step], F32(0.5), F32(1.0))
        re = damp * re
        im = damp * im
        if step == STEPS - 1:
            at = pl.ds(b * bs, bs)
            final[0, at, :] = re
            final[1, at, :] = im
        else:
            put_w(w_bufs[1 - step % 2], b, re.astype(BF16), im.astype(BF16))

    for grp in range(len(cuts) - 1):
        for which in range(2):
            load_copy(which, grp).wait()
        load_start(grp + AHEAD)
        if grp == MEET:
            pl.semaphore_wait(barrier, depth_n - 1 + len(near_peers) + len(far_peers))
            halo_start(0)
        if cuts[grp + 1] == nb:
            halo_finish(0)
            multiply(0, 0)
            multiply(0, nb - 1)
        for b in range(max(cuts[grp], 1), min(cuts[grp + 1], nb - 1)):
            multiply(0, b)
    halo_start(1)
    for step in range(1, STEPS):
        middle = nb // 2
        for b in range(1, middle):
            multiply(step, b)
        halo_finish(step)
        multiply(step, 0)
        multiply(step, nb - 1)
        for b in range(middle, nb - 1):
            multiply(step, b)
        if step + 1 < STEPS:
            halo_start(step + 1)

    limit = jnp.uint32(rows)

    def pick(owner, dst, chunk):
        start, count = chunks[chunk]

        def one(j, carry):
            spot = receivers[owner * here + start + j] - first_row
            spot = jnp.minimum(spot.astype(jnp.uint32), limit).astype(jnp.int32)
            for c in range(2):
                dst[c, pl.ds(start + j, 1), :] = final[c, pl.ds(spot, 1), :]
            return carry
        lax.fori_loop(0, count, one, 0, unroll=16)

    def pick_copy(off, chunk):
        return pltpu.make_async_remote_copy(
            src_ref=pick_out.at[off - 1, chunk],
            dst_ref=pick_in.at[off - 1, chunk],
            send_sem=pick_send.at[off - 1, chunk],
            recv_sem=pick_recv.at[off - 1, chunk],
            device_id={"depth": lax.rem(me_d + off, depth_n)},
            device_id_type=MESH,
        )

    for off in range(1, depth_n):
        for chunk, (start, count) in enumerate(chunks):
            pick(lax.rem(me_d + off, depth_n), rows_f32.at[off], chunk)
            pick_out[off - 1, chunk] = rows_f32[off, :, start:start + count, :].astype(BF16)
            pick_copy(off, chunk).start()
    for chunk in range(len(chunks)):
        pick(me_d, rows_f32.at[0], chunk)

    def ag_copy(off, chunk):
        return pltpu.make_async_remote_copy(
            src_ref=gathered.at[0, chunk],
            dst_ref=gathered.at[off, chunk],
            send_sem=ag_send.at[off - 1, chunk],
            recv_sem=ag_recv.at[off - 1, chunk],
            device_id={"freq": near_peers[off - 1]},
            device_id_type=MESH,
        )

    for chunk, (start, count) in enumerate(chunks):
        at = slice(start, start + count)
        mine = rows_f32[0, :, at, :]
        for off in range(1, depth_n):
            pick_copy(off, chunk).wait()
            mine = mine + pick_in[off - 1, chunk].astype(F32)
        gathered[0, chunk] = mine.astype(BF16)
        for off in range(1, near):
            ag_copy(off, chunk).start()

    def rs_copy(off, chunk):
        start, count = chunks[chunk]
        at = pl.ds(start, count)
        return pltpu.make_async_remote_copy(
            src_ref=part_out.at[off - 1, at],
            dst_ref=part_in.at[off - 1, at],
            send_sem=rs_send.at[off - 1, chunk],
            recv_sem=rs_recv.at[off - 1, chunk],
            device_id={"freq": far_peers[off - 1]},
            device_id_type=MESH,
        )

    for chunk, (start, count) in enumerate(chunks):
        at = slice(start, start + count)
        for off in range(1, near):
            ag_copy(off, chunk).wait_recv()
        lhs = jnp.concatenate([gathered[slot, chunk, c] for slot in range(near) for c in range(2)], axis=1)
        rhs = jnp.concatenate([basis[slot] for slot in range(near)], axis=0)
        total = jnp.dot(lhs, rhs, preferred_element_type=F32)
        for off in range(1, far):
            part_out[off - 1, at, :] = total[:, off * times:(off + 1) * times].astype(BF16)
            rs_copy(off, chunk).start()
        kept[at, :] = total[:, :times]
    for chunk, (start, count) in enumerate(chunks):
        at = slice(start, start + count)
        total = kept[at, :]
        for off in range(1, far):
            rs_copy(off, chunk).wait_recv()
            total = total + part_in[off - 1, at, :].astype(F32)
        out[at, :] = total * factor
    for chunk in range(len(chunks)):
        for off in range(1, near):
            ag_copy(off, chunk).wait_send()
        for off in range(1, far):
            rs_copy(off, chunk).wait_send()


def local(depth_n, freq_n, pressure_field, block_main, block_coupled, coupling, frequencies,
          receivers, floors):
    rows, width = pressure_field.shape
    bs = block_main.shape[3]
    half = width // 2
    nb = rows // bs
    near = min(4, freq_n)
    far = freq_n // near
    here = receivers.shape[0] // depth_n
    times = NT // freq_n
    factor = 1.0 / math.sqrt(frequencies.shape[0])
    count = max(here // 4, 16)
    chunks = [(start, count) for start in range(0, here, count)]
    vmem = pl.BlockSpec(memory_space=pltpu.VMEM)
    hbm = pl.BlockSpec(memory_space=pltpu.HBM)
    smem = pl.BlockSpec(memory_space=pltpu.SMEM)
    away = max(depth_n - 1, 1)
    near_slots, far_slots = max(near - 1, 1), max(far - 1, 1)
    dma = pltpu.SemaphoreType.DMA
    return pl.pallas_call(
        functools.partial(kernel, depth_n, freq_n, near, factor, chunks),
        out_shape=jax.ShapeDtypeStruct((here, times), F32),
        in_specs=[hbm, hbm, hbm, vmem, vmem, smem, smem],
        out_specs=vmem,
        scratch_shapes=[
            pltpu.VMEM((rows, width), BF16),
            pltpu.VMEM((rows * KC, bs), BF16),
            pltpu.VMEM((rows * KC, bs), BF16),
            pltpu.VMEM((nb, KC, 2 * bs, bs), BF16),
            pltpu.VMEM((3, rows, half), BF16),
            pltpu.VMEM((3, rows, half), BF16),
            pltpu.VMEM((2, rows + 8, half), F32),
            pltpu.VMEM((STEPS, 2, 3, bs, half), BF16),
            pltpu.VMEM((depth_n, 2, here, half), F32),
            pltpu.VMEM((away, len(chunks), 2, count, half), BF16),
            pltpu.VMEM((away, len(chunks), 2, count, half), BF16),
            pltpu.VMEM((near, len(chunks), 2, count, half), BF16),
            pltpu.VMEM((near, width, NT // near), BF16),
            pltpu.VMEM((here, times), F32),
            pltpu.VMEM((far_slots, here, times), BF16),
            pltpu.VMEM((far_slots, here, times), BF16),
            dma((FIELD_PARTS,)),
            dma((2, len(group_cuts(nb)) - 1)),
            dma((STEPS, 2)),
            dma((STEPS, 2)),
            dma((away, len(chunks))),
            dma((away, len(chunks))),
            dma((near_slots, len(chunks))),
            dma((near_slots, len(chunks))),
            dma((far_slots, len(chunks))),
            dma((far_slots, len(chunks))),
        ],
        compiler_params=pltpu.CompilerParams(
            collective_id=0, has_side_effects=True, vmem_limit_bytes=VMEM_LIMIT
        ),
    )(*(pltpu.with_memory_space_constraint(x, pltpu.HBM) for x in (
        pressure_field,
        block_main.reshape(rows * KC, bs),
        block_coupled.reshape(rows * KC, bs),
        coupling.reshape(2, half),
        frequencies.reshape(freq_n, half),
        receivers,
        floors,
    )))


def solution(mesh):
    in_specs = (
        P("depth", "freq"),
        P("depth", None, None, None),
        P("depth", None, None, None),
        P("freq"),
        P(),
        P(),
        P(),
    )
    body = functools.partial(local, mesh.shape["depth"], mesh.shape["freq"])
    return jax.shard_map(body, mesh=mesh, in_specs=in_specs, out_specs=P("depth", "freq"),
                         check_vma=False)
```

```python
import functools
import math

import jax
import jax.numpy as jnp
from jax import lax
from jax.experimental import pallas as pl
from jax.experimental.pallas import tpu as pltpu
from jax.sharding import PartitionSpec as P

NT = 2048
STEPS = 4

COS_TERMS = (1.0, -19.739208221435547, 64.93939208984375, -85.45665740966797,
             60.242130279541016, -26.4046688079834, 7.800131320953369, -1.453112244606018)
SIN_TERMS = (6.2831854820251465, -41.34170150756836, 81.6052474975586, -76.70580291748047,
             42.05775451660156, -15.086565017700195, 3.7813189029693604, -0.6207787394523621)

MESH = pl.DeviceIdType.MESH
F32 = jnp.float32
BF16 = jnp.bfloat16
KC = 6
VMEM_LIMIT = 46 * 1024 * 1024
GROUPS = (4, 8, 8, 8, 4)
MEET = 3
CHUNKS = ((0, 5), (5, 5), (10, 4), (14, 2))
AHEAD = 3
FIELD_PARTS = 8


def poly(terms, z):
    total = jnp.full_like(z, terms[-1])
    for term in terms[-2::-1]:
        total = total * z + F32(term)
    return total


def group_cuts(nb):
    cuts = [0]
    while cuts[-1] < nb:
        cuts.append(min(nb, cuts[-1] + GROUPS[min(len(cuts) - 1, len(GROUPS) - 1)]))
    return cuts


def kernel(depth_n, freq_n, near, factor, chunks,
           field, main_hbm, side_hbm, coupling_hbm, freqs_hbm, receivers_hbm, floors_hbm, out,
           coupling, freqs, receivers, floors, fbuf, raw_main, raw_side, ops, w_even, w_odd, final, halo, rows_f32, pick_out, pick_in,
           gathered, basis, kept, part_out, part_in,
           small_sem, field_sem, load_sem, halo_send, halo_recv, pick_send, pick_recv, ag_send, ag_recv, rs_send, rs_recv):
    rows, width = fbuf.shape
    half = width // 2
    nb, _, bw, bs = ops.shape
    cuts = group_cuts(nb)
    far = freq_n // near
    here, times = out.shape
    wide = NT // near
    me_d = lax.axis_index("depth")
    me_f = lax.axis_index("freq")
    me_near = lax.rem(me_f, near)
    me_far = me_f // near
    first_row = me_d * rows
    has_above = me_d > 0
    has_below = me_d < depth_n - 1
    w_bufs = (w_even, w_odd)

    def field_copy(part):
        at = pl.ds(part * (rows // FIELD_PARTS), rows // FIELD_PARTS)
        return pltpu.make_async_copy(field.at[at], fbuf.at[at], field_sem)

    for part in range(FIELD_PARTS):
        field_copy(part).start()

    def load_start(grp):
        if grp < len(cuts) - 1:
            for which in range(2):
                load_copy(which, grp).start()

    def load_copy(which, grp):
        src, dst = ((main_hbm, raw_main), (side_hbm, raw_side))[which]
        at = pl.ds(cuts[grp] * bs * KC, (cuts[grp + 1] - cuts[grp]) * bs * KC)
        return pltpu.make_async_copy(src.at[at], dst.at[at], load_sem.at[which, grp])

    smalls = [
        pltpu.make_async_copy(src, dst, small_sem.at[i])
        for i, (src, dst) in enumerate(((coupling_hbm, coupling), (floors_hbm, floors),
                                        (freqs_hbm, freqs), (receivers_hbm, receivers)))
    ]
    for copy in smalls:
        copy.start()
    load_start(0)

    near_peers = []
    for off in range(1, near):
        peer = me_f
        for bit in range(near.bit_length() - 1):
            if off >> bit & 1:
                mine = lax.rem(me_f // (1 << bit), 2)
                peer = peer + (1 - 2 * mine) * (1 << bit)
        near_peers.append(peer)
    far_peers = [lax.rem(me_far + off, far) * near + me_near for off in range(1, far)]
    barrier = pltpu.get_barrier_semaphore()
    for off in range(1, depth_n):
        pl.semaphore_signal(barrier, inc=1, device_id={"depth": lax.rem(me_d + off, depth_n)},
                            device_id_type=MESH)
    for peer in near_peers + far_peers:
        pl.semaphore_signal(barrier, inc=1, device_id={"freq": peer}, device_id_type=MESH)

    load_start(1)

    from_col = lax.broadcasted_iota(jnp.int32, (width, width), 0)
    to_col = lax.broadcasted_iota(jnp.int32, (width, width), 1)
    wanted = jnp.where(to_col < half, 2 * to_col, 2 * (to_col - half) + 1)
    order = jnp.where(from_col == wanted, 1.0, 0.0).astype(BF16)

    smalls[0].wait()
    pairs = jnp.broadcast_to(jnp.concatenate([coupling[0:1, :], coupling[1:2, :]], axis=1), (16, width))
    weights = jnp.zeros((16, width), F32)
    rest = pairs
    for _ in range(3):
        piece = rest.astype(BF16)
        weights = weights + jnp.dot(piece, order, preferred_element_type=F32)
        rest = rest - piece.astype(F32)
    wr = weights[0:1, :half]
    wi = weights[0:1, half:]

    def put_w(dst, b, re, im):
        at = pl.ds(b * bs, bs)
        dst[0, at, :] = re
        dst[1, at, :] = im
        dst[2, at, :] = -im

    blank = jnp.zeros(halo.shape[2:], BF16)

    @pl.when(jnp.logical_not(has_above))
    def _():
        for step in range(STEPS):
            halo[step, 0] = blank

    @pl.when(jnp.logical_not(has_below))
    def _():
        for step in range(STEPS):
            halo[step, 1] = blank

    final[:, rows:, :] = jnp.zeros((2, final.shape[1] - rows, half), F32)

    for copy in smalls[1:]:
        copy.wait()
    pltpu.make_async_copy(field, fbuf, field_sem).wait()
    load_start(AHEAD - 1)

    def enter(b):
        at = pl.ds(b * bs, bs)
        got = jnp.dot(fbuf[at, :], order, preferred_element_type=F32).astype(BF16)
        put_w(w_even, b, got[:, :half], got[:, half:])

    for b in [0, nb - 1] + list(range(1, nb - 1)):
        enter(b)

    def halo_copy(step, side):
        edge = 0 if side == 1 else nb - 1
        to = lax.rem(me_d + (depth_n - 1 if side == 1 else 1), depth_n)
        return pltpu.make_async_remote_copy(
            src_ref=w_bufs[step % 2].at[:, pl.ds(edge * bs, bs)],
            dst_ref=halo.at[step, side],
            send_sem=halo_send.at[step % 2, side],
            recv_sem=halo_recv.at[step % 2, side],
            device_id={"depth": to},
            device_id_type=MESH,
        )

    def halo_start(step):
        if depth_n == 1:
            return

        @pl.when(has_above)
        def _():
            halo_copy(step, 1).start()

        @pl.when(has_below)
        def _():
            halo_copy(step, 0).start()

    def halo_finish(step):
        if depth_n == 1:
            return

        @pl.when(has_above)
        def _():
            halo_copy(step, 1).wait_send()
            halo_copy(step, 0).wait_recv()

        @pl.when(has_below)
        def _():
            halo_copy(step, 0).wait_send()
            halo_copy(step, 1).wait_recv()

    row_iota = lax.broadcasted_iota(jnp.int32, (bs, half), 0)

    def multiply(step, b):
        src = w_bufs[step % 2]
        pieces = []
        for k in range(3):
            at = b + k - 1
            if at < 0:
                re, im, neg = (halo[step, 0, c] for c in range(3))
            elif at >= nb:
                re, im, neg = (halo[step, 1, c] for c in range(3))
            else:
                re, im, neg = (src[c, pl.ds(at * bs, bs), :] for c in range(3))
            pieces.append(jnp.concatenate([re, im], axis=1))
            pieces.append(jnp.concatenate([neg, re], axis=1))
        rhs = jnp.concatenate(pieces, axis=0)
        if step == 0:
            lhs = jnp.concatenate([
                jnp.concatenate([raw[pl.ds(b * KC * bs + piece, bs, stride=KC), :] for piece in range(KC)], axis=1)
                for raw in (raw_main, raw_side)
            ], axis=0)
            for piece in range(KC):
                ops[b, piece] = lhs[:, piece * bs:(piece + 1) * bs]
        else:
            lhs = jnp.concatenate([ops[b, piece] for piece in range(KC)], axis=1)
        acc = jnp.dot(lhs, rhs, preferred_element_type=F32)
        m, c = acc[:bs], acc[bs:]
        re = m[:, :half] + wr * c[:, :half] - wi * c[:, half:]
        im = m[:, half:] + wr * c[:, half:] + wi * c[:, :half]
        damp = jnp.where(row_iota + (first_row + b * bs) >= floors[step], F32(0.5), F32(1.0))
        re = damp * re
        im = damp * im
        if step == STEPS - 1:
            at = pl.ds(b * bs, bs)
            final[0, at, :] = re
            final[1, at, :] = im
        else:
            put_w(w_bufs[1 - step % 2], b, re.astype(BF16), im.astype(BF16))

    for grp in range(len(cuts) - 1):
        for which in range(2):
            load_copy(which, grp).wait()
        load_start(grp + AHEAD)
        if grp == MEET:
            pl.semaphore_wait(barrier, depth_n - 1 + len(near_peers) + len(far_peers))
            halo_start(0)
        if cuts[grp + 1] == nb:
            halo_finish(0)
            multiply(0, 0)
            multiply(0, nb - 1)
        for b in range(max(cuts[grp], 1), min(cuts[grp + 1], nb - 1)):
            multiply(0, b)
    halo_start(1)
    for step in range(1, STEPS):
        middle = nb // 2
        for b in range(1, middle):
            multiply(step, b)
        halo_finish(step)
        multiply(step, 0)
        multiply(step, nb - 1)
        for b in range(middle, nb - 1):
            multiply(step, b)
        if step + 1 < STEPS:
            halo_start(step + 1)

    limit = jnp.uint32(rows)

    def pick(owner, dst, chunk):
        start, count = chunks[chunk]

        def one(j, carry):
            spot = receivers[owner * here + start + j] - first_row
            spot = jnp.minimum(spot.astype(jnp.uint32), limit).astype(jnp.int32)
            for c in range(2):
                dst[c, pl.ds(start + j, 1), :] = final[c, pl.ds(spot, 1), :]
            return carry
        lax.fori_loop(0, count, one, 0, unroll=16)

    def pick_copy(off, at, chunk):
        return pltpu.make_async_remote_copy(
            src_ref=pick_out.at[off - 1, :, at],
            dst_ref=pick_in.at[off - 1, :, at],
            send_sem=pick_send.at[off - 1],
            recv_sem=pick_recv.at[off - 1, chunk],
            device_id={"depth": lax.rem(me_d + off, depth_n)},
            device_id_type=MESH,
        )

    for off in range(1, depth_n):
        for chunk, (start, count) in enumerate(chunks):
            pick(lax.rem(me_d + off, depth_n), rows_f32.at[off], chunk)
            pick_out[off - 1, :, start:start + count, :] = rows_f32[off, :, start:start + count, :].astype(BF16)
            pick_copy(off, pl.ds(start, count), chunk).start()
    for chunk in range(len(chunks)):
        pick(me_d, rows_f32.at[0], chunk)

    def ag_copy(off, at, chunk):
        return pltpu.make_async_remote_copy(
            src_ref=gathered.at[0, :, at],
            dst_ref=gathered.at[off, :, at],
            send_sem=ag_send,
            recv_sem=ag_recv.at[chunk],
            device_id={"freq": near_peers[off - 1]},
            device_id_type=MESH,
        )

    def ag_all(at, chunk):
        others = gathered.at[pl.ds(1, near - 1), :, at]
        return pltpu.make_async_remote_copy(
            src_ref=others,
            dst_ref=others,
            send_sem=ag_send,
            recv_sem=ag_recv.at[chunk],
            device_id={"freq": near_peers[0]},
            device_id_type=MESH,
        )

    for chunk, (start, count) in enumerate(chunks):
        at = slice(start, start + count)
        mine = rows_f32[0, :, at, :]
        for off in range(1, depth_n):
            pick_copy(off, pl.ds(start, count), chunk).wait_recv()
            mine = mine + pick_in[off - 1, :, at, :].astype(F32)
        gathered[0, :, at, :] = mine.astype(BF16)
        for off in range(near - 1, 0, -1):
            ag_copy(off, pl.ds(start, count), chunk).start()

    lane = lax.broadcasted_iota(jnp.int32, (half, wide), 1)
    owner = lax.rem(lane // times + me_far, far)
    sample = ((owner * near + me_near) * times + lax.rem(lane, times)).astype(F32)
    for slot, peer in enumerate([me_f] + near_peers):
        row = freqs[pl.ds(peer, 1), :]
        column = jnp.broadcast_to(row, (half, half)).T
        for start in range(0, wide, half):
            n = sample[:, start:start + half]
            y = (column[:, :n.shape[1]] * n) * F32(1.0 / NT)
            p = y - jnp.floor(y)
            r = jnp.where(p > 0.5, p - 1.0, p)
            z = r * r
            basis[slot, :half, start:start + half] = poly(COS_TERMS, z).astype(BF16)
            basis[slot, half:, start:start + half] = (-(r * poly(SIN_TERMS, z))).astype(BF16)

    def rs_copy(off, at, chunk):
        return pltpu.make_async_remote_copy(
            src_ref=part_out.at[off - 1, at],
            dst_ref=part_in.at[off - 1, at],
            send_sem=rs_send,
            recv_sem=rs_recv.at[chunk],
            device_id={"freq": far_peers[off - 1]},
            device_id_type=MESH,
        )

    def rs_all(at, chunk):
        return pltpu.make_async_remote_copy(
            src_ref=part_out.at[:, at],
            dst_ref=part_in.at[:, at],
            send_sem=rs_send,
            recv_sem=rs_recv.at[chunk],
            device_id={"freq": far_peers[0]},
            device_id_type=MESH,
        )

    for chunk, (start, count) in enumerate(chunks):
        at = slice(start, start + count)
        if near > 1:
            ag_all(pl.ds(start, count), chunk).wait_recv()
        lhs = jnp.concatenate([gathered[slot, c, at, :] for slot in range(near) for c in range(2)], axis=1)
        rhs = jnp.concatenate([basis[slot] for slot in range(near)], axis=0)
        total = jnp.dot(lhs, rhs, preferred_element_type=F32)
        for off in range(1, far):
            part_out[off - 1, at, :] = total[:, off * times:(off + 1) * times].astype(BF16)
            rs_copy(off, pl.ds(start, count), chunk).start()
        kept[at, :] = total[:, :times]
    for chunk, (start, count) in enumerate(chunks):
        at = slice(start, start + count)
        total = kept[at, :]
        if far > 1:
            rs_all(pl.ds(start, count), chunk).wait_recv()
        for off in range(1, far):
            total = total + part_in[off - 1, at, :].astype(F32)
        out[at, :] = total * factor
    everything = pl.ds(0, here)
    for off in range(1, depth_n):
        pick_copy(off, everything, 0).wait_send()
    if near > 1:
        ag_all(everything, 0).wait_send()
    if far > 1:
        rs_all(everything, 0).wait_send()


def local(depth_n, freq_n, pressure_field, block_main, block_coupled, coupling, frequencies,
          receivers, floors):
    rows, width = pressure_field.shape
    bs = block_main.shape[3]
    half = width // 2
    nb = rows // bs
    near = min(4, freq_n)
    far = freq_n // near
    here = receivers.shape[0] // depth_n
    times = NT // freq_n
    factor = 1.0 / math.sqrt(frequencies.shape[0])
    unit = here // 16
    chunks = [(start * unit, size * unit) for start, size in CHUNKS]
    vmem = pl.BlockSpec(memory_space=pltpu.VMEM)
    hbm = pl.BlockSpec(memory_space=pltpu.HBM)
    away = max(depth_n - 1, 1)
    far_slots = max(far - 1, 1)
    dma = pltpu.SemaphoreType.DMA
    return pl.pallas_call(
        functools.partial(kernel, depth_n, freq_n, near, factor, chunks),
        out_shape=jax.ShapeDtypeStruct((here, times), F32),
        in_specs=[hbm] * 7,
        out_specs=vmem,
        scratch_shapes=[
            pltpu.VMEM((2, half), F32),
            pltpu.VMEM((freq_n, half), F32),
            pltpu.SMEM(receivers.shape, jnp.int32),
            pltpu.SMEM(floors.shape, jnp.int32),
            pltpu.VMEM((rows, width), BF16),
            pltpu.VMEM((rows * KC, bs), BF16),
            pltpu.VMEM((rows * KC, bs), BF16),
            pltpu.VMEM((nb, KC, 2 * bs, bs), BF16),
            pltpu.VMEM((3, rows, half), BF16),
            pltpu.VMEM((3, rows, half), BF16),
            pltpu.VMEM((2, rows + 8, half), F32),
            pltpu.VMEM((STEPS, 2, 3, bs, half), BF16),
            pltpu.VMEM((depth_n, 2, here, half), F32),
            pltpu.VMEM((away, 2, here, half), BF16),
            pltpu.VMEM((away, 2, here, half), BF16),
            pltpu.VMEM((near, 2, here, half), BF16),
            pltpu.VMEM((near, width, NT // near), BF16),
            pltpu.VMEM((here, times), F32),
            pltpu.VMEM((far_slots, here, times), BF16),
            pltpu.VMEM((far_slots, here, times), BF16),
            dma((4,)),
            dma(()),
            dma((2, len(group_cuts(nb)) - 1)),
            dma((2, 2)),
            dma((2, 2)),
            dma((away,)),
            dma((away, len(chunks))),
            dma(()),
            dma((len(chunks),)),
            dma(()),
            dma((len(chunks),)),
        ],
        compiler_params=pltpu.CompilerParams(
            collective_id=0, has_side_effects=True, vmem_limit_bytes=VMEM_LIMIT
        ),
    )(*(pltpu.with_memory_space_constraint(x, pltpu.HBM) for x in (
        pressure_field,
        block_main.reshape(rows * KC, bs),
        block_coupled.reshape(rows * KC, bs),
        coupling.reshape(2, half),
        frequencies.reshape(freq_n, half),
        receivers,
        floors,
    )))


def solution(mesh):
    in_specs = (
        P("depth", "freq"),
        P("depth", None, None, None),
        P("depth", None, None, None),
        P("freq"),
        P(),
        P(),
        P(),
    )
    body = functools.partial(local, mesh.shape["depth"], mesh.shape["freq"])
    return jax.shard_map(body, mesh=mesh, in_specs=in_specs, out_specs=P("depth", "freq"),
                         check_vma=False)
```

```python
import functools
import math

import jax
import jax.numpy as jnp
from jax import lax
from jax.experimental import pallas as pl
from jax.experimental.pallas import tpu as pltpu
from jax.sharding import PartitionSpec as P

NT = 2048
STEPS = 4

COS_TERMS = (1.0, -19.739208221435547, 64.93939208984375, -85.45665740966797,
             60.242130279541016, -26.4046688079834, 7.800131320953369, -1.453112244606018)
SIN_TERMS = (6.2831854820251465, -41.34170150756836, 81.6052474975586, -76.70580291748047,
             42.05775451660156, -15.086565017700195, 3.7813189029693604, -0.6207787394523621)

MESH = pl.DeviceIdType.MESH
F32 = jnp.float32
BF16 = jnp.bfloat16
KC = 6
VMEM_LIMIT = 46 * 1024 * 1024
GROUPS = (4, 8, 8, 8, 4)
MEET = 3
EXTRA = 5
UNITS = 16
AHEAD = 3
FIELD_PARTS = 8


def poly(terms, z):
    total = jnp.full_like(z, terms[-1])
    for term in terms[-2::-1]:
        total = total * z + F32(term)
    return total


def group_cuts(nb):
    cuts = [0]
    while cuts[-1] < nb:
        cuts.append(min(nb, cuts[-1] + GROUPS[min(len(cuts) - 1, len(GROUPS) - 1)]))
    return cuts


def kernel(depth_n, freq_n, near, factor, chunks, extra,
           field, main_hbm, side_hbm, coupling_hbm, freqs_hbm, receivers_hbm, floors_hbm, out,
           coupling, freqs, receivers, floors, fbuf, raw_main, raw_side, ops, w_even, w_odd, final, halo, rows_f32, pick_out, pick_in,
           gathered, basis, kept, part_out, part_in,
           result_out, result_in, result_send, result_recv, small_sem, field_sem, load_sem, halo_send, halo_recv, pick_send, pick_recv, ag_send, ag_recv, rs_send, rs_recv):
    rows, width = fbuf.shape
    half = width // 2
    nb, _, bw, bs = ops.shape
    cuts = group_cuts(nb)
    far = freq_n // near
    here, times = out.shape
    wide = NT // near
    me_d = lax.axis_index("depth")
    me_f = lax.axis_index("freq")
    me_near = lax.rem(me_f, near)
    me_far = me_f // near
    first_row = me_d * rows
    has_above = me_d > 0
    has_below = me_d < depth_n - 1
    w_bufs = (w_even, w_odd)

    def field_copy(part):
        at = pl.ds(part * (rows // FIELD_PARTS), rows // FIELD_PARTS)
        return pltpu.make_async_copy(field.at[at], fbuf.at[at], field_sem)

    for part in range(FIELD_PARTS):
        field_copy(part).start()

    def load_start(grp):
        if grp < len(cuts) - 1:
            for which in range(2):
                load_copy(which, grp).start()

    def load_copy(which, grp):
        src, dst = ((main_hbm, raw_main), (side_hbm, raw_side))[which]
        at = pl.ds(cuts[grp] * bs * KC, (cuts[grp + 1] - cuts[grp]) * bs * KC)
        return pltpu.make_async_copy(src.at[at], dst.at[at], load_sem.at[which, grp])

    smalls = [
        pltpu.make_async_copy(src, dst, small_sem.at[i])
        for i, (src, dst) in enumerate(((coupling_hbm, coupling), (floors_hbm, floors),
                                        (freqs_hbm, freqs), (receivers_hbm, receivers)))
    ]
    for copy in smalls:
        copy.start()
    load_start(0)

    near_peers = []
    for off in range(1, near):
        peer = me_f
        for bit in range(near.bit_length() - 1):
            if off >> bit & 1:
                mine = lax.rem(me_f // (1 << bit), 2)
                peer = peer + (1 - 2 * mine) * (1 << bit)
        near_peers.append(peer)
    far_peers = [lax.rem(me_far + off, far) * near + me_near for off in range(1, far)]
    barrier = pltpu.get_barrier_semaphore()
    for off in range(1, depth_n):
        pl.semaphore_signal(barrier, inc=1, device_id={"depth": lax.rem(me_d + off, depth_n)},
                            device_id_type=MESH)
    for peer in near_peers + far_peers:
        pl.semaphore_signal(barrier, inc=1, device_id={"freq": peer}, device_id_type=MESH)

    load_start(1)

    from_col = lax.broadcasted_iota(jnp.int32, (width, width), 0)
    to_col = lax.broadcasted_iota(jnp.int32, (width, width), 1)
    wanted = jnp.where(to_col < half, 2 * to_col, 2 * (to_col - half) + 1)
    order = jnp.where(from_col == wanted, 1.0, 0.0).astype(BF16)

    smalls[0].wait()
    pairs = jnp.broadcast_to(jnp.concatenate([coupling[0:1, :], coupling[1:2, :]], axis=1), (16, width))
    weights = jnp.zeros((16, width), F32)
    rest = pairs
    for _ in range(3):
        piece = rest.astype(BF16)
        weights = weights + jnp.dot(piece, order, preferred_element_type=F32)
        rest = rest - piece.astype(F32)
    wr = weights[0:1, :half]
    wi = weights[0:1, half:]

    def put_w(dst, b, re, im):
        at = pl.ds(b * bs, bs)
        dst[0, at, :] = re
        dst[1, at, :] = im
        dst[2, at, :] = -im

    blank = jnp.zeros(halo.shape[2:], BF16)

    @pl.when(jnp.logical_not(has_above))
    def _():
        for step in range(STEPS):
            halo[step, 0] = blank

    @pl.when(jnp.logical_not(has_below))
    def _():
        for step in range(STEPS):
            halo[step, 1] = blank

    final[:, rows:, :] = jnp.zeros((2, final.shape[1] - rows, half), F32)

    for copy in smalls[1:]:
        copy.wait()
    pltpu.make_async_copy(field, fbuf, field_sem).wait()
    load_start(AHEAD - 1)

    def enter(b):
        at = pl.ds(b * bs, bs)
        got = jnp.dot(fbuf[at, :], order, preferred_element_type=F32).astype(BF16)
        put_w(w_even, b, got[:, :half], got[:, half:])

    for b in [0, nb - 1] + list(range(1, nb - 1)):
        enter(b)

    def halo_copy(step, side):
        edge = 0 if side == 1 else nb - 1
        to = lax.rem(me_d + (depth_n - 1 if side == 1 else 1), depth_n)
        return pltpu.make_async_remote_copy(
            src_ref=w_bufs[step % 2].at[:, pl.ds(edge * bs, bs)],
            dst_ref=halo.at[step, side],
            send_sem=halo_send.at[step % 2, side],
            recv_sem=halo_recv.at[step % 2, side],
            device_id={"depth": to},
            device_id_type=MESH,
        )

    def halo_start(step):
        if depth_n == 1:
            return

        @pl.when(has_above)
        def _():
            halo_copy(step, 1).start()

        @pl.when(has_below)
        def _():
            halo_copy(step, 0).start()

    def halo_finish(step):
        if depth_n == 1:
            return

        @pl.when(has_above)
        def _():
            halo_copy(step, 1).wait_send()
            halo_copy(step, 0).wait_recv()

        @pl.when(has_below)
        def _():
            halo_copy(step, 0).wait_send()
            halo_copy(step, 1).wait_recv()

    row_iota = lax.broadcasted_iota(jnp.int32, (bs, half), 0)

    def multiply(step, b):
        src = w_bufs[step % 2]
        pieces = []
        for k in range(3):
            at = b + k - 1
            if at < 0:
                re, im, neg = (halo[step, 0, c] for c in range(3))
            elif at >= nb:
                re, im, neg = (halo[step, 1, c] for c in range(3))
            else:
                re, im, neg = (src[c, pl.ds(at * bs, bs), :] for c in range(3))
            pieces.append(jnp.concatenate([re, im], axis=1))
            pieces.append(jnp.concatenate([neg, re], axis=1))
        rhs = jnp.concatenate(pieces, axis=0)
        if step == 0:
            lhs = jnp.concatenate([
                jnp.concatenate([raw[pl.ds(b * KC * bs + piece, bs, stride=KC), :] for piece in range(KC)], axis=1)
                for raw in (raw_main, raw_side)
            ], axis=0)
            for piece in range(KC):
                ops[b, piece] = lhs[:, piece * bs:(piece + 1) * bs]
        else:
            lhs = jnp.concatenate([ops[b, piece] for piece in range(KC)], axis=1)
        acc = jnp.dot(lhs, rhs, preferred_element_type=F32)
        m, c = acc[:bs], acc[bs:]
        re = m[:, :half] + wr * c[:, :half] - wi * c[:, half:]
        im = m[:, half:] + wr * c[:, half:] + wi * c[:, :half]
        damp = jnp.where(row_iota + (first_row + b * bs) >= floors[step], F32(0.5), F32(1.0))
        re = damp * re
        im = damp * im
        if step == STEPS - 1:
            at = pl.ds(b * bs, bs)
            final[0, at, :] = re
            final[1, at, :] = im
        else:
            put_w(w_bufs[1 - step % 2], b, re.astype(BF16), im.astype(BF16))

    for grp in range(len(cuts) - 1):
        for which in range(2):
            load_copy(which, grp).wait()
        load_start(grp + AHEAD)
        if grp == MEET:
            pl.semaphore_wait(barrier, depth_n - 1 + len(near_peers) + len(far_peers))
            halo_start(0)
        if cuts[grp + 1] == nb:
            halo_finish(0)
            multiply(0, 0)
            multiply(0, nb - 1)
        for b in range(max(cuts[grp], 1), min(cuts[grp + 1], nb - 1)):
            multiply(0, b)
    halo_start(1)
    for step in range(1, STEPS):
        middle = nb // 2
        for b in range(1, middle):
            multiply(step, b)
        halo_finish(step)
        multiply(step, 0)
        multiply(step, nb - 1)
        for b in range(middle, nb - 1):
            multiply(step, b)
        if step + 1 < STEPS:
            halo_start(step + 1)

    limit = jnp.uint32(rows)

    heavy, light = me_d == depth_n - 1, me_d == 0
    shared = here - extra

    def by(who, kind, body):
        if kind == "both":
            body()
        else:
            pl.when(who)(body)

    def pick(base, dst, start, count):
        def one(j, carry):
            spot = receivers[base + j] - first_row
            spot = jnp.minimum(spot.astype(jnp.uint32), limit).astype(jnp.int32)
            for c in range(2):
                dst[c, pl.ds(start + j, 1), :] = final[c, pl.ds(spot, 1), :]
            return carry
        lax.fori_loop(0, count, one, 0, unroll=16)

    def base_of(kind, owner, start):
        return shared if kind == "moved" else owner * here + start

    def pick_copy(off, at, chunk):
        return pltpu.make_async_remote_copy(
            src_ref=pick_out.at[off - 1, :, at],
            dst_ref=pick_in.at[off - 1, :, at],
            send_sem=pick_send.at[off - 1],
            recv_sem=pick_recv.at[off - 1, chunk],
            device_id={"depth": lax.rem(me_d + off, depth_n)},
            device_id_type=MESH,
        )

    for off in range(1, depth_n):
        for chunk, (start, count, kind) in enumerate(chunks):
            def give(off=off, chunk=chunk, start=start, count=count, kind=kind):
                pick(base_of(kind, lax.rem(me_d + off, depth_n), start), rows_f32.at[off], start, count)
                pick_out[off - 1, :, start:start + count, :] = rows_f32[off, :, start:start + count, :].astype(BF16)
                pick_copy(off, pl.ds(start, count), chunk).start()
            by(light, kind, give)
    for chunk, (start, count, kind) in enumerate(chunks):
        def take(start=start, count=count, kind=kind):
            pick(base_of(kind, me_d, start), rows_f32.at[0], start, count)
        by(heavy, kind, take)

    def ag_copy(off, at, chunk):
        return pltpu.make_async_remote_copy(
            src_ref=gathered.at[0, :, at],
            dst_ref=gathered.at[off, :, at],
            send_sem=ag_send,
            recv_sem=ag_recv.at[chunk],
            device_id={"freq": near_peers[off - 1]},
            device_id_type=MESH,
        )

    def ag_all(at, chunk):
        others = gathered.at[pl.ds(1, near - 1), :, at]
        return pltpu.make_async_remote_copy(
            src_ref=others,
            dst_ref=others,
            send_sem=ag_send,
            recv_sem=ag_recv.at[chunk],
            device_id={"freq": near_peers[0]},
            device_id_type=MESH,
        )

    for chunk, (start, count, kind) in enumerate(chunks):
        def spread(chunk=chunk, start=start, count=count):
            at = slice(start, start + count)
            mine = rows_f32[0, :, at, :]
            for off in range(1, depth_n):
                pick_copy(off, pl.ds(start, count), chunk).wait_recv()
                mine = mine + pick_in[off - 1, :, at, :].astype(F32)
            gathered[0, :, at, :] = mine.astype(BF16)
            for off in range(near - 1, 0, -1):
                ag_copy(off, pl.ds(start, count), chunk).start()
        by(heavy, kind, spread)

    lane = lax.broadcasted_iota(jnp.int32, (half, wide), 1)
    owner = lax.rem(lane // times + me_far, far)
    sample = ((owner * near + me_near) * times + lax.rem(lane, times)).astype(F32)
    for slot, peer in enumerate([me_f] + near_peers):
        row = freqs[pl.ds(peer, 1), :]
        column = jnp.broadcast_to(row, (half, half)).T
        for start in range(0, wide, half):
            n = sample[:, start:start + half]
            y = (column[:, :n.shape[1]] * n) * F32(1.0 / NT)
            p = y - jnp.floor(y)
            r = jnp.where(p > 0.5, p - 1.0, p)
            z = r * r
            basis[slot, :half, start:start + half] = poly(COS_TERMS, z).astype(BF16)
            basis[slot, half:, start:start + half] = (-(r * poly(SIN_TERMS, z))).astype(BF16)

    def rs_copy(off, at, chunk):
        return pltpu.make_async_remote_copy(
            src_ref=part_out.at[off - 1, at],
            dst_ref=part_in.at[off - 1, at],
            send_sem=rs_send,
            recv_sem=rs_recv.at[chunk],
            device_id={"freq": far_peers[off - 1]},
            device_id_type=MESH,
        )

    def rs_all(at, chunk):
        return pltpu.make_async_remote_copy(
            src_ref=part_out.at[:, at],
            dst_ref=part_in.at[:, at],
            send_sem=rs_send,
            recv_sem=rs_recv.at[chunk],
            device_id={"freq": far_peers[0]},
            device_id_type=MESH,
        )

    for chunk, (start, count, kind) in enumerate(chunks):
        def synthesize(chunk=chunk, start=start, count=count):
            at = slice(start, start + count)
            if near > 1:
                ag_all(pl.ds(start, count), chunk).wait_recv()
            lhs = jnp.concatenate([gathered[slot, c, at, :] for slot in range(near) for c in range(2)], axis=1)
            rhs = jnp.concatenate([basis[slot] for slot in range(near)], axis=0)
            total = jnp.dot(lhs, rhs, preferred_element_type=F32)
            for off in range(1, far):
                part_out[off - 1, at, :] = total[:, off * times:(off + 1) * times].astype(BF16)
                rs_copy(off, pl.ds(start, count), chunk).start()
            kept[at, :] = total[:, :times]
        by(heavy, kind, synthesize)

    result_copy = pltpu.make_async_remote_copy(
        src_ref=result_out,
        dst_ref=result_in,
        send_sem=result_send,
        recv_sem=result_recv,
        device_id={"depth": 0},
        device_id_type=MESH,
    )
    for chunk, (start, count, kind) in enumerate(chunks):
        def finish(chunk=chunk, start=start, count=count, kind=kind):
            at = slice(start, start + count)
            total = kept[at, :]
            if far > 1:
                rs_all(pl.ds(start, count), chunk).wait_recv()
            for off in range(1, far):
                total = total + part_in[off - 1, at, :].astype(F32)
            if kind == "moved":
                result_out[...] = total * factor
                result_copy.start()
            else:
                out[at, :] = total * factor
        by(heavy, kind, finish)

    def close(sent, owned):
        for off in range(1, depth_n):
            pick_copy(off, pl.ds(0, sent), 0).wait_send()
        if near > 1:
            ag_all(pl.ds(0, owned), 0).wait_send()
        if far > 1:
            rs_all(pl.ds(0, owned), 0).wait_send()

    if not extra:
        close(here, here)
        return

    @pl.when(heavy)
    def _():
        result_copy.wait_send()
        close(shared, here + extra)

    @pl.when(light)
    def _():
        result_copy.wait_recv()
        out[shared:, :] = result_in[...]
        close(here + extra, shared)


def local(depth_n, freq_n, pressure_field, block_main, block_coupled, coupling, frequencies,
          receivers, floors):
    rows, width = pressure_field.shape
    bs = block_main.shape[3]
    half = width // 2
    nb = rows // bs
    near = min(4, freq_n)
    far = freq_n // near
    here = receivers.shape[0] // depth_n
    times = NT // freq_n
    factor = 1.0 / math.sqrt(frequencies.shape[0])
    unit = here // UNITS
    extra = EXTRA * unit if depth_n == 2 else 0
    room = here + extra
    shared = (here - extra) // unit
    cuts = [0, shared * 3 // 8, shared * 6 // 8, shared]
    chunks = [(lo * unit, (hi - lo) * unit, "both") for lo, hi in zip(cuts, cuts[1:])]
    if extra:
        chunks.insert(1, (here, extra, "moved"))
        chunks.insert(3, (here - extra, extra, "own"))
    vmem = pl.BlockSpec(memory_space=pltpu.VMEM)
    hbm = pl.BlockSpec(memory_space=pltpu.HBM)
    away = max(depth_n - 1, 1)
    far_slots = max(far - 1, 1)
    dma = pltpu.SemaphoreType.DMA
    return pl.pallas_call(
        functools.partial(kernel, depth_n, freq_n, near, factor, chunks, extra),
        out_shape=jax.ShapeDtypeStruct((here, times), F32),
        in_specs=[hbm] * 7,
        out_specs=vmem,
        scratch_shapes=[
            pltpu.VMEM((2, half), F32),
            pltpu.VMEM((freq_n, half), F32),
            pltpu.SMEM(receivers.shape, jnp.int32),
            pltpu.SMEM(floors.shape, jnp.int32),
            pltpu.VMEM((rows, width), BF16),
            pltpu.VMEM((rows * KC, bs), BF16),
            pltpu.VMEM((rows * KC, bs), BF16),
            pltpu.VMEM((nb, KC, 2 * bs, bs), BF16),
            pltpu.VMEM((3, rows, half), BF16),
            pltpu.VMEM((3, rows, half), BF16),
            pltpu.VMEM((2, rows + 8, half), F32),
            pltpu.VMEM((STEPS, 2, 3, bs, half), BF16),
            pltpu.VMEM((depth_n, 2, room, half), F32),
            pltpu.VMEM((away, 2, room, half), BF16),
            pltpu.VMEM((away, 2, room, half), BF16),
            pltpu.VMEM((near, 2, room, half), BF16),
            pltpu.VMEM((near, width, NT // near), BF16),
            pltpu.VMEM((room, times), F32),
            pltpu.VMEM((far_slots, room, times), BF16),
            pltpu.VMEM((far_slots, room, times), BF16),
            pltpu.VMEM((max(extra, 8), times), F32),
            pltpu.VMEM((max(extra, 8), times), F32),
            dma(()),
            dma(()),
            dma((4,)),
            dma(()),
            dma((2, len(group_cuts(nb)) - 1)),
            dma((2, 2)),
            dma((2, 2)),
            dma((away,)),
            dma((away, len(chunks))),
            dma(()),
            dma((len(chunks),)),
            dma(()),
            dma((len(chunks),)),
        ],
        compiler_params=pltpu.CompilerParams(
            collective_id=0, has_side_effects=True, vmem_limit_bytes=VMEM_LIMIT
        ),
    )(*(pltpu.with_memory_space_constraint(x, pltpu.HBM) for x in (
        pressure_field,
        block_main.reshape(rows * KC, bs),
        block_coupled.reshape(rows * KC, bs),
        coupling.reshape(2, half),
        frequencies.reshape(freq_n, half),
        receivers,
        floors,
    )))


def solution(mesh):
    in_specs = (
        P("depth", "freq"),
        P("depth", None, None, None),
        P("depth", None, None, None),
        P("freq"),
        P(),
        P(),
        P(),
    )
    body = functools.partial(local, mesh.shape["depth"], mesh.shape["freq"])
    return jax.shard_map(body, mesh=mesh, in_specs=in_specs, out_specs=P("depth", "freq"),
                         check_vma=False)
```

```python
import functools
import math

import jax
import jax.numpy as jnp
from jax import lax
from jax.experimental import pallas as pl
from jax.experimental.pallas import tpu as pltpu
from jax.sharding import PartitionSpec as P

NT = 2048
STEPS = 4

COS_TERMS = (1.0, -19.739208221435547, 64.93939208984375, -85.45665740966797,
             60.242130279541016, -26.4046688079834, 7.800131320953369, -1.453112244606018)
SIN_TERMS = (6.2831854820251465, -41.34170150756836, 81.6052474975586, -76.70580291748047,
             42.05775451660156, -15.086565017700195, 3.7813189029693604, -0.6207787394523621)

MESH = pl.DeviceIdType.MESH
F32 = jnp.float32
BF16 = jnp.bfloat16
KC = 6
VMEM_LIMIT = 46 * 1024 * 1024
GROUPS = (4, 8, 8, 8, 4)
MEET = 3
EXTRA = 6
UNITS = 16
AHEAD = 3
FIELD_PARTS = 8


def poly(terms, z):
    total = jnp.full_like(z, terms[-1])
    for term in terms[-2::-1]:
        total = total * z + F32(term)
    return total


def group_cuts(nb):
    cuts = [0]
    while cuts[-1] < nb:
        cuts.append(min(nb, cuts[-1] + GROUPS[min(len(cuts) - 1, len(GROUPS) - 1)]))
    return cuts


def kernel(depth_n, freq_n, near, factor, chunks, extra,
           field, main_hbm, side_hbm, coupling_hbm, freqs_hbm, receivers_hbm, floors_hbm, out,
           coupling, freqs, receivers, floors, fbuf, raw_main, raw_side, ops, w_even, w_odd, final, halo, rows_f32, pick_out, pick_in,
           gathered, basis, kept, part_out, part_in,
           result_out, result_in, result_send, result_recv, small_sem, field_sem, load_sem, halo_send, halo_recv, pick_send, pick_recv, ag_send, ag_recv, rs_send, rs_recv):
    rows, width = fbuf.shape
    half = width // 2
    nb, _, bw, bs = ops.shape
    cuts = group_cuts(nb)
    far = freq_n // near
    here, times = out.shape
    wide = NT // near
    me_d = lax.axis_index("depth")
    me_f = lax.axis_index("freq")
    me_near = lax.rem(me_f, near)
    me_far = me_f // near
    first_row = me_d * rows
    has_above = me_d > 0
    has_below = me_d < depth_n - 1
    w_bufs = (w_even, w_odd)

    def field_copy(part):
        at = pl.ds(part * (rows // FIELD_PARTS), rows // FIELD_PARTS)
        return pltpu.make_async_copy(field.at[at], fbuf.at[at], field_sem)

    for part in range(FIELD_PARTS):
        field_copy(part).start()

    def load_start(grp):
        if grp < len(cuts) - 1:
            for which in range(2):
                load_copy(which, grp).start()

    def load_copy(which, grp):
        src, dst = ((main_hbm, raw_main), (side_hbm, raw_side))[which]
        at = pl.ds(cuts[grp] * bs * KC, (cuts[grp + 1] - cuts[grp]) * bs * KC)
        return pltpu.make_async_copy(src.at[at], dst.at[at], load_sem.at[which, grp])

    smalls = [
        pltpu.make_async_copy(src, dst, small_sem.at[i])
        for i, (src, dst) in enumerate(((coupling_hbm, coupling), (floors_hbm, floors),
                                        (freqs_hbm, freqs), (receivers_hbm, receivers)))
    ]
    for copy in smalls:
        copy.start()
    load_start(0)

    near_peers = []
    for off in range(1, near):
        peer = me_f
        for bit in range(near.bit_length() - 1):
            if off >> bit & 1:
                mine = lax.rem(me_f // (1 << bit), 2)
                peer = peer + (1 - 2 * mine) * (1 << bit)
        near_peers.append(peer)
    far_peers = [lax.rem(me_far + off, far) * near + me_near for off in range(1, far)]
    barrier = pltpu.get_barrier_semaphore()
    for off in range(1, depth_n):
        pl.semaphore_signal(barrier, inc=1, device_id={"depth": lax.rem(me_d + off, depth_n)},
                            device_id_type=MESH)
    for peer in near_peers + far_peers:
        pl.semaphore_signal(barrier, inc=1, device_id={"freq": peer}, device_id_type=MESH)

    load_start(1)

    from_col = lax.broadcasted_iota(jnp.int32, (width, width), 0)
    to_col = lax.broadcasted_iota(jnp.int32, (width, width), 1)
    wanted = jnp.where(to_col < half, 2 * to_col, 2 * (to_col - half) + 1)
    order = jnp.where(from_col == wanted, 1.0, 0.0).astype(BF16)

    smalls[0].wait()
    pairs = jnp.broadcast_to(jnp.concatenate([coupling[0:1, :], coupling[1:2, :]], axis=1), (16, width))
    weights = jnp.zeros((16, width), F32)
    rest = pairs
    for _ in range(3):
        piece = rest.astype(BF16)
        weights = weights + jnp.dot(piece, order, preferred_element_type=F32)
        rest = rest - piece.astype(F32)
    wr = weights[0:1, :half]
    wi = weights[0:1, half:]

    def put_w(dst, b, re, im):
        at = pl.ds(b * bs, bs)
        dst[0, at, :] = re
        dst[1, at, :] = im
        dst[2, at, :] = -im

    blank = jnp.zeros(halo.shape[2:], BF16)

    @pl.when(jnp.logical_not(has_above))
    def _():
        for step in range(STEPS):
            halo[step, 0] = blank

    @pl.when(jnp.logical_not(has_below))
    def _():
        for step in range(STEPS):
            halo[step, 1] = blank

    final[:, rows:, :] = jnp.zeros((2, final.shape[1] - rows, half), F32)

    for copy in smalls[1:]:
        copy.wait()
    pltpu.make_async_copy(field, fbuf, field_sem).wait()
    load_start(AHEAD - 1)

    def enter(b):
        at = pl.ds(b * bs, bs)
        got = jnp.dot(fbuf[at, :], order, preferred_element_type=F32).astype(BF16)
        put_w(w_even, b, got[:, :half], got[:, half:])

    for b in [0, nb - 1] + list(range(1, nb - 1)):
        enter(b)

    def halo_copy(step, side):
        edge = 0 if side == 1 else nb - 1
        to = lax.rem(me_d + (depth_n - 1 if side == 1 else 1), depth_n)
        return pltpu.make_async_remote_copy(
            src_ref=w_bufs[step % 2].at[:, pl.ds(edge * bs, bs)],
            dst_ref=halo.at[step, side],
            send_sem=halo_send.at[step % 2, side],
            recv_sem=halo_recv.at[step % 2, side],
            device_id={"depth": to},
            device_id_type=MESH,
        )

    def halo_start(step):
        if depth_n == 1:
            return

        @pl.when(has_above)
        def _():
            halo_copy(step, 1).start()

        @pl.when(has_below)
        def _():
            halo_copy(step, 0).start()

    def halo_finish(step):
        if depth_n == 1:
            return

        @pl.when(has_above)
        def _():
            halo_copy(step, 1).wait_send()
            halo_copy(step, 0).wait_recv()

        @pl.when(has_below)
        def _():
            halo_copy(step, 0).wait_send()
            halo_copy(step, 1).wait_recv()

    row_iota = lax.broadcasted_iota(jnp.int32, (bs, half), 0)

    def multiply(step, b):
        src = w_bufs[step % 2]
        pieces = []
        for k in range(3):
            at = b + k - 1
            if at < 0:
                re, im, neg = (halo[step, 0, c] for c in range(3))
            elif at >= nb:
                re, im, neg = (halo[step, 1, c] for c in range(3))
            else:
                re, im, neg = (src[c, pl.ds(at * bs, bs), :] for c in range(3))
            pieces.append(jnp.concatenate([re, im], axis=1))
            pieces.append(jnp.concatenate([neg, re], axis=1))
        rhs = jnp.concatenate(pieces, axis=0)
        if step == 0:
            lhs = jnp.concatenate([
                jnp.concatenate([raw[pl.ds(b * KC * bs + piece, bs, stride=KC), :] for piece in range(KC)], axis=1)
                for raw in (raw_main, raw_side)
            ], axis=0)
            for piece in range(KC):
                ops[b, piece] = lhs[:, piece * bs:(piece + 1) * bs]
        else:
            lhs = jnp.concatenate([ops[b, piece] for piece in range(KC)], axis=1)
        acc = jnp.dot(lhs, rhs, preferred_element_type=F32)
        m, c = acc[:bs], acc[bs:]
        re = m[:, :half] + wr * c[:, :half] - wi * c[:, half:]
        im = m[:, half:] + wr * c[:, half:] + wi * c[:, :half]
        damp = jnp.where(row_iota + (first_row + b * bs) >= floors[step], F32(0.5), F32(1.0))
        re = damp * re
        im = damp * im
        if step == STEPS - 1:
            at = pl.ds(b * bs, bs)
            final[0, at, :] = re
            final[1, at, :] = im
        else:
            put_w(w_bufs[1 - step % 2], b, re.astype(BF16), im.astype(BF16))

    for grp in range(len(cuts) - 1):
        for which in range(2):
            load_copy(which, grp).wait()
        load_start(grp + AHEAD)
        if grp == MEET:
            pl.semaphore_wait(barrier, depth_n - 1 + len(near_peers) + len(far_peers))
            halo_start(0)
        if cuts[grp + 1] == nb:
            halo_finish(0)
            multiply(0, 0)
            multiply(0, nb - 1)
        for b in range(max(cuts[grp], 1), min(cuts[grp + 1], nb - 1)):
            multiply(0, b)
    halo_start(1)
    for step in range(1, STEPS):
        middle = nb // 2
        for b in range(1, middle):
            multiply(step, b)
        halo_finish(step)
        multiply(step, 0)
        multiply(step, nb - 1)
        for b in range(middle, nb - 1):
            multiply(step, b)
        if step + 1 < STEPS:
            halo_start(step + 1)

    limit = jnp.uint32(rows)

    heavy, light = me_d == depth_n - 1, me_d == 0
    shared = here - extra

    def by(who, kind, body):
        if kind == "both":
            body()
        else:
            pl.when(who)(body)

    def pick(base, dst, start, count):
        def one(j, carry):
            spot = receivers[base + j] - first_row
            spot = jnp.minimum(spot.astype(jnp.uint32), limit).astype(jnp.int32)
            for c in range(2):
                dst[c, pl.ds(start + j, 1), :] = final[c, pl.ds(spot, 1), :]
            return carry
        lax.fori_loop(0, count, one, 0, unroll=16)

    def base_of(kind, owner, start):
        return shared if kind == "moved" else owner * here + start

    def pick_copy(off, at, chunk):
        return pltpu.make_async_remote_copy(
            src_ref=pick_out.at[off - 1, :, at],
            dst_ref=pick_in.at[off - 1, :, at],
            send_sem=pick_send.at[off - 1],
            recv_sem=pick_recv.at[off - 1, chunk],
            device_id={"depth": lax.rem(me_d + off, depth_n)},
            device_id_type=MESH,
        )

    for off in range(1, depth_n):
        for chunk, (start, count, kind) in enumerate(chunks):
            def give(off=off, chunk=chunk, start=start, count=count, kind=kind):
                pick(base_of(kind, lax.rem(me_d + off, depth_n), start), rows_f32.at[off], start, count)
                pick_out[off - 1, :, start:start + count, :] = rows_f32[off, :, start:start + count, :].astype(BF16)
                pick_copy(off, pl.ds(start, count), chunk).start()
            by(light, kind, give)
    for chunk, (start, count, kind) in enumerate(chunks):
        def take(start=start, count=count, kind=kind):
            pick(base_of(kind, me_d, start), rows_f32.at[0], start, count)
        by(heavy, kind, take)

    def ag_copy(off, at, chunk):
        return pltpu.make_async_remote_copy(
            src_ref=gathered.at[0, :, at],
            dst_ref=gathered.at[off, :, at],
            send_sem=ag_send,
            recv_sem=ag_recv.at[chunk],
            device_id={"freq": near_peers[off - 1]},
            device_id_type=MESH,
        )

    def ag_all(at, chunk):
        others = gathered.at[pl.ds(1, near - 1), :, at]
        return pltpu.make_async_remote_copy(
            src_ref=others,
            dst_ref=others,
            send_sem=ag_send,
            recv_sem=ag_recv.at[chunk],
            device_id={"freq": near_peers[0]},
            device_id_type=MESH,
        )

    for chunk, (start, count, kind) in enumerate(chunks):
        def spread(chunk=chunk, start=start, count=count):
            at = slice(start, start + count)
            mine = rows_f32[0, :, at, :]
            for off in range(1, depth_n):
                pick_copy(off, pl.ds(start, count), chunk).wait_recv()
                mine = mine + pick_in[off - 1, :, at, :].astype(F32)
            gathered[0, :, at, :] = mine.astype(BF16)
            for off in range(near - 1, 0, -1):
                ag_copy(off, pl.ds(start, count), chunk).start()
        by(heavy, kind, spread)

    lane = lax.broadcasted_iota(jnp.int32, (half, wide), 1)
    owner = lax.rem(lane // times + me_far, far)
    sample = ((owner * near + me_near) * times + lax.rem(lane, times)).astype(F32)
    for slot, peer in enumerate([me_f] + near_peers):
        row = freqs[pl.ds(peer, 1), :]
        column = jnp.broadcast_to(row, (half, half)).T
        for start in range(0, wide, half):
            n = sample[:, start:start + half]
            y = (column[:, :n.shape[1]] * n) * F32(1.0 / NT)
            p = y - jnp.floor(y)
            r = jnp.where(p > 0.5, p - 1.0, p)
            z = r * r
            basis[slot, :half, start:start + half] = poly(COS_TERMS, z).astype(BF16)
            basis[slot, half:, start:start + half] = (-(r * poly(SIN_TERMS, z))).astype(BF16)

    def rs_copy(off, at, chunk):
        return pltpu.make_async_remote_copy(
            src_ref=part_out.at[off - 1, at],
            dst_ref=part_in.at[off - 1, at],
            send_sem=rs_send,
            recv_sem=rs_recv.at[chunk],
            device_id={"freq": far_peers[off - 1]},
            device_id_type=MESH,
        )

    def rs_all(at, chunk):
        return pltpu.make_async_remote_copy(
            src_ref=part_out.at[:, at],
            dst_ref=part_in.at[:, at],
            send_sem=rs_send,
            recv_sem=rs_recv.at[chunk],
            device_id={"freq": far_peers[0]},
            device_id_type=MESH,
        )

    for chunk, (start, count, kind) in enumerate(chunks):
        def synthesize(chunk=chunk, start=start, count=count):
            at = slice(start, start + count)
            if near > 1:
                ag_all(pl.ds(start, count), chunk).wait_recv()
            lhs = jnp.concatenate([gathered[slot, c, at, :] for slot in range(near) for c in range(2)], axis=1)
            rhs = jnp.concatenate([basis[slot] for slot in range(near)], axis=0)
            total = jnp.dot(lhs, rhs, preferred_element_type=F32)
            for off in range(1, far):
                part_out[off - 1, at, :] = total[:, off * times:(off + 1) * times].astype(BF16)
                rs_copy(off, pl.ds(start, count), chunk).start()
            kept[at, :] = total[:, :times]
        by(heavy, kind, synthesize)

    result_copy = pltpu.make_async_remote_copy(
        src_ref=result_out,
        dst_ref=result_in,
        send_sem=result_send,
        recv_sem=result_recv,
        device_id={"depth": 0},
        device_id_type=MESH,
    )
    for chunk, (start, count, kind) in enumerate(chunks):
        def finish(chunk=chunk, start=start, count=count, kind=kind):
            at = slice(start, start + count)
            total = kept[at, :]
            if far > 1:
                rs_all(pl.ds(start, count), chunk).wait_recv()
            for off in range(1, far):
                total = total + part_in[off - 1, at, :].astype(F32)
            if kind == "moved":
                result_out[...] = total * factor
                result_copy.start()
            else:
                out[at, :] = total * factor
        by(heavy, kind, finish)

    def close(sent, owned):
        for off in range(1, depth_n):
            pick_copy(off, pl.ds(0, sent), 0).wait_send()
        if near > 1:
            ag_all(pl.ds(0, owned), 0).wait_send()
        if far > 1:
            rs_all(pl.ds(0, owned), 0).wait_send()

    if not extra:
        close(here, here)
        return

    @pl.when(heavy)
    def _():
        result_copy.wait_send()
        close(shared, here + extra)

    @pl.when(light)
    def _():
        result_copy.wait_recv()
        out[shared:, :] = result_in[...]
        close(here + extra, shared)


def local(depth_n, freq_n, pressure_field, block_main, block_coupled, coupling, frequencies,
          receivers, floors):
    rows, width = pressure_field.shape
    bs = block_main.shape[3]
    half = width // 2
    nb = rows // bs
    near = min(4, freq_n)
    far = freq_n // near
    here = receivers.shape[0] // depth_n
    times = NT // freq_n
    factor = 1.0 / math.sqrt(frequencies.shape[0])
    unit = here // UNITS
    extra = EXTRA * unit if depth_n == 2 else 0
    room = here + extra
    shared = (here - extra) // unit
    cuts = [0, shared * 2 // 5, shared * 4 // 5, shared]
    chunks = [(lo * unit, (hi - lo) * unit, "both") for lo, hi in zip(cuts, cuts[1:])]
    if extra:
        chunks.insert(1, (here, extra, "moved"))
        chunks.insert(3, (here - extra, extra, "own"))
    vmem = pl.BlockSpec(memory_space=pltpu.VMEM)
    hbm = pl.BlockSpec(memory_space=pltpu.HBM)
    away = max(depth_n - 1, 1)
    far_slots = max(far - 1, 1)
    dma = pltpu.SemaphoreType.DMA
    return pl.pallas_call(
        functools.partial(kernel, depth_n, freq_n, near, factor, chunks, extra),
        out_shape=jax.ShapeDtypeStruct((here, times), F32),
        in_specs=[hbm] * 7,
        out_specs=vmem,
        scratch_shapes=[
            pltpu.VMEM((2, half), F32),
            pltpu.VMEM((freq_n, half), F32),
            pltpu.SMEM(receivers.shape, jnp.int32),
            pltpu.SMEM(floors.shape, jnp.int32),
            pltpu.VMEM((rows, width), BF16),
            pltpu.VMEM((rows * KC, bs), BF16),
            pltpu.VMEM((rows * KC, bs), BF16),
            pltpu.VMEM((nb, KC, 2 * bs, bs), BF16),
            pltpu.VMEM((3, rows, half), BF16),
            pltpu.VMEM((3, rows, half), BF16),
            pltpu.VMEM((2, rows + 8, half), F32),
            pltpu.VMEM((STEPS, 2, 3, bs, half), BF16),
            pltpu.VMEM((depth_n, 2, room, half), F32),
            pltpu.VMEM((away, 2, room, half), BF16),
            pltpu.VMEM((away, 2, room, half), BF16),
            pltpu.VMEM((near, 2, room, half), BF16),
            pltpu.VMEM((near, width, NT // near), BF16),
            pltpu.VMEM((room, times), F32),
            pltpu.VMEM((far_slots, room, times), BF16),
            pltpu.VMEM((far_slots, room, times), BF16),
            pltpu.VMEM((max(extra, 8), times), F32),
            pltpu.VMEM((max(extra, 8), times), F32),
            dma(()),
            dma(()),
            dma((4,)),
            dma(()),
            dma((2, len(group_cuts(nb)) - 1)),
            dma((2, 2)),
            dma((2, 2)),
            dma((away,)),
            dma((away, len(chunks))),
            dma(()),
            dma((len(chunks),)),
            dma(()),
            dma((len(chunks),)),
        ],
        compiler_params=pltpu.CompilerParams(
            collective_id=0, has_side_effects=True, vmem_limit_bytes=VMEM_LIMIT
        ),
    )(*(pltpu.with_memory_space_constraint(x, pltpu.HBM) for x in (
        pressure_field,
        block_main.reshape(rows * KC, bs),
        block_coupled.reshape(rows * KC, bs),
        coupling.reshape(2, half),
        frequencies.reshape(freq_n, half),
        receivers,
        floors,
    )))


def solution(mesh):
    in_specs = (
        P("depth", "freq"),
        P("depth", None, None, None),
        P("depth", None, None, None),
        P("freq"),
        P(),
        P(),
        P(),
    )
    body = functools.partial(local, mesh.shape["depth"], mesh.shape["freq"])
    return jax.shard_map(body, mesh=mesh, in_specs=in_specs, out_specs=P("depth", "freq"),
                         check_vma=False)
```
